32 devices in a mesh: cell: 2 (over x), row: 8 (over z, y), col: 2 (over core).
Axes of the slice: x: 2, y: 2, z: 4, core: 2. Of those that a mesh axis runs over, the one named last changes fastest.
Arguments:
- half_system: bfloat16 [32768, 32768], P(('cell', 'row'), 'col'), parts along dimension 0, may hold values from -6 to 6
- vectors: bfloat16 [65536, 512], P(('cell', 'col', 'row')), parts along dimension 0, may hold values from -0.03125 to 0.03125
- edge: bfloat16 [512, 64, 512], P(('cell', 'row'), None, 'col'), parts along dimension 0, may hold values from -6 to 6
- ket: bfloat16 [128, 128], P('cell'), parts along dimension 0, may hold values from -0.5 to 0.5
- bra: bfloat16 [128, 128], P('cell'), parts along dimension 0, may hold values from -0.75 to 0.75
Outputs:
- new_edge: bfloat16 [1024, 64, 512], P(('cell', 'row'), None, 'col'), parts along dimension 0
The draws below stay inside these ranges and needn't reach their ends.
There are 2 independent parts, one for each index of `cell`. The reference program is written for one: setup_inputs(seed, part) draws one part's arguments, and reference() takes and returns one part's arrays. A program takes and returns all parts, laid end to end along the dimension named above; each array names one. Nothing has to cross between parts.
All inputs are finite; a program needn't handle non-finite values.
Results may differ from the reference program's by a relative error of at most 0.0076.
Values may be sent and summed in bfloat16 or wider, within the bound.
No kernel may reach another device: no remote copies, remote signals or barrier semaphores. Data moves between devices by JAX's collectives and lax.ppermute only.
A program may use at most 128 MiB of HBM per device.

```python
import jax
import jax.numpy as jnp

CHI = 512
D2 = 64
CL = 256
LEGS = 128
K = 32768
KR = 16384


def shard_levels(own_key, dims, shards, low, largest):
    level, own = 1.0, jax.random.fold_in(own_key, 6)
    for axis_at, parts in shards:
        heights = jnp.exp(jax.random.uniform(jax.random.fold_in(own, axis_at), (parts,), jnp.float32, low / len(shards), largest / len(shards)))
        level = level * jnp.repeat(heights, dims[axis_at] // parts).reshape([-1 if axis == axis_at else 1 for axis in range(len(dims))])
    return level


def noise(key, shape, spread, reach, cuts=(), kind=jnp.bfloat16):
    values = jax.random.normal(key, shape, jnp.float32) * spread
    if len(cuts) > 0:
        values = shard_levels(key, shape, cuts, -0.22, 0.18) * values
    return jnp.clip(values, min=-reach, max=reach).astype(kind)


def setup_inputs(seed: int = 0, part: int = 0) -> dict:
    streams_of = jax.random.split(jax.random.key(seed), 6)
    part_keys = jax.random.split(jax.random.fold_in(streams_of[5], part), 6)
    half_system = noise(part_keys[0], (KR, K), 1.0, 6.0, ((0, 8), (1, 2)))
    vectors = noise(part_keys[1], (K, CHI), K ** -0.5, 0.03125, ((0, 16),))
    edge = noise(part_keys[2], (CL, D2, CHI), 1.0, 6.0, ((0, 8), (2, 2)))
    ket = noise(part_keys[3], (D2, LEGS), LEGS ** -0.5, 0.5)
    bra = noise(part_keys[4], (D2, LEGS), D2 ** -0.5, 0.75)
    return {"half_system": half_system, "vectors": vectors, "edge": edge, "ket": ket, "bra": bra}


def reference(half_system, vectors, edge, ket, bra):
    projector = jnp.dot(half_system, vectors, preferred_element_type=jnp.float32).astype(jnp.bfloat16)
    layer = jnp.dot(ket, bra.T, preferred_element_type=jnp.float32).astype(jnp.bfloat16)
    absorbed = jnp.einsum('aub,us->asb', edge.astype(jnp.float32), layer.astype(jnp.float32)).astype(jnp.bfloat16)
    proj3 = projector.reshape(CL, D2, CHI)
    middle = jnp.einsum('asc,asb->scb', proj3.astype(jnp.float32), absorbed.astype(jnp.float32))
    middle = (middle * (CL ** -0.5)).astype(jnp.bfloat16)
    new_edge = jnp.einsum('ts,scb->ctb', layer.astype(jnp.float32), middle.astype(jnp.float32))
    return new_edge.astype(jnp.bfloat16)
```

```python
import jax
import jax.numpy as jnp
from jax import lax
from jax.experimental import pallas as pl
from jax.experimental.pallas import tpu as pltpu
from jax.sharding import PartitionSpec as P


SWAP = [(0, 1), (1, 0)]
KERNEL_VMEM = 32 << 20
KEPT, SENT, BLOCKS = 0, 1, 2


def held(half_system, table, index, depth, pieces):
    rows = half_system.shape[0]

    def kernel(table_ref, from_ref, to_ref, sems):
        copies = [
            pltpu.make_async_copy(
                from_ref.at[pl.ds(i * (rows // pieces), rows // pieces), pl.ds(table_ref[index] * depth, depth)],
                to_ref.at[pl.ds(i * (rows // pieces), rows // pieces), :],
                sems.at[i],
            )
            for i in range(pieces)
        ]
        for copy in copies:
            copy.start()
        for copy in copies:
            copy.wait()

    return pl.pallas_call(
        kernel,
        in_specs=[pl.BlockSpec(memory_space=pltpu.SMEM), pl.BlockSpec(memory_space=pl.ANY)],
        out_specs=pl.BlockSpec(memory_space=pltpu.VMEM),
        out_shape=pltpu.VMEM((rows, depth), half_system.dtype),
        scratch_shapes=[pltpu.SemaphoreType.DMA((pieces,))],
        compiler_params=pltpu.CompilerParams(vmem_limit_bytes=KERNEL_VMEM),
    )(table, half_system)


def block_dots(half_system, table, at, depth, jobs, part=None, last=None):
    rows = half_system.shape[0]
    count = len(at)
    width = next(block.shape[1] for block in jobs[0][1] if block is not None)
    out_rows = rows if part is None else rows // 2
    tile = min(out_rows, 512 if part is None else 1024)
    steps = out_rows // tile

    def first_tile(table):
        return 0 if part is None else table[part] * steps

    if last is None:
        specs = [
            pl.BlockSpec((tile, depth), lambda m, table, i=i: (first_tile(table) + m, table[i])) for i in at
        ]
        operands = [half_system] * count
    else:
        specs, operands = [pl.BlockSpec(memory_space=pltpu.VMEM)], [last]
    plan, aliases = [], {}
    for o, (total, blocks) in enumerate(jobs):
        terms = []
        for i, block in enumerate(blocks):
            if block is not None:
                terms.append((i, len(specs)))
                specs.append(pl.BlockSpec((depth, width), lambda m, table: (0, 0)))
                operands.append(block)
        plan.append((terms, None if total is None else len(specs)))
        if total is not None:
            if part is None:
                aliases[len(operands) + 1] = o
            specs.append(pl.BlockSpec(memory_space=pltpu.VMEM))
            operands.append(total)

    def kernel(table_ref, *refs):
        here = pl.ds(pl.multiple_of(pl.program_id(0) * tile, tile), tile)
        there = pl.ds(pl.multiple_of((first_tile(table_ref) + pl.program_id(0)) * tile, tile), tile)
        for (terms, total_at), out_ref in zip(plan, refs[len(specs) :]):
            value = None if total_at is None else refs[total_at][there, :]
            for i, j in terms:
                left = refs[i][...] if last is None else refs[i][there, :]
                term = jnp.dot(left, refs[j][...], preferred_element_type=jnp.float32)
                value = term if value is None else value + term
            if part is None:
                out_ref[here, :] = value
            else:
                out_ref[...] = value

    terms = sum(len(p[0]) for p in plan)
    if part is None:
        out_specs = [pl.BlockSpec(memory_space=pltpu.VMEM) for _ in jobs]
        out_shape = [pltpu.VMEM((out_rows, width), jnp.float32) for _ in jobs]
    else:
        out_specs = [pl.BlockSpec((tile, width), lambda m, table: (m, 0)) for _ in jobs]
        out_shape = [jax.ShapeDtypeStruct((out_rows, width), jnp.float32) for _ in jobs]
    return pl.pallas_call(
        kernel,
        grid_spec=pltpu.PrefetchScalarGridSpec(
            num_scalar_prefetch=1, grid=(steps,), in_specs=specs, out_specs=out_specs
        ),
        out_shape=out_shape,
        input_output_aliases=aliases,
        compiler_params=pltpu.CompilerParams(vmem_limit_bytes=KERNEL_VMEM),
        cost_estimate=pl.CostEstimate(
            flops=2 * out_rows * width * depth * terms,
            bytes_accessed=2 * count * out_rows * depth + 2 * terms * depth * width,
            transcendentals=0,
        ),
    )(table, *operands)


def middle_of(table, row_count, moved, other, moved_edge, scale):
    layers = moved.shape[0] // row_count
    left, width = moved.shape[1:]
    right = moved_edge.shape[2]
    per_row = width // row_count

    def grouped(value):
        return value.reshape(row_count, layers, *value.shape[1:])

    steps = 1
    group = layers // steps

    def kernel(table_ref, moved_ref, other_ref, mine_ref, theirs_ref, out_ref):
        for s in range(group):
            p = jnp.concatenate([ref[:, s].reshape(row_count * left, width) for ref in (moved_ref, other_ref)])
            e = jnp.concatenate([ref[:, s].reshape(row_count * left, right) for ref in (mine_ref, theirs_ref)])
            value = lax.dot_general(p, e, (((0,), (0,)), ((), ())), preferred_element_type=jnp.float32) * scale
            out_ref[:, s] = value.astype(jnp.bfloat16).reshape(row_count, per_row, right)

    block = pl.BlockSpec((row_count, group, left, width), lambda s, table: (0, s, 0, 0))
    out = pl.pallas_call(
        kernel,
        grid_spec=pltpu.PrefetchScalarGridSpec(
            num_scalar_prefetch=1,
            grid=(steps,),
            in_specs=[
                block,
                block,
                pl.BlockSpec((row_count, group, left, right), lambda s, table: (0, s, table[KEPT], 0)),
                pl.BlockSpec((row_count, group, left, right), lambda s, table: (0, s, table[SENT], 0)),
            ],
            out_specs=pl.BlockSpec((row_count, group, per_row, right), lambda s, table: (0, s, 0, 0)),
        ),
        out_shape=jax.ShapeDtypeStruct((row_count, layers, per_row, right), jnp.bfloat16),
        compiler_params=pltpu.CompilerParams(vmem_limit_bytes=KERNEL_VMEM),
    )(table, grouped(moved), grouped(other), grouped(moved_edge), grouped(moved_edge))
    return out.reshape(row_count * layers, per_row, right)


def plain(half_system, vectors, edge, ket, bra):
    partial_value = jnp.dot(
        half_system, lax.all_gather(vectors, "row", axis=0, tiled=True), preferred_element_type=jnp.float32
    )
    projector = lax.psum_scatter(partial_value, "col", scatter_dimension=1, tiled=True).astype(jnp.bfloat16)
    layer = jnp.dot(ket, bra.T, preferred_element_type=jnp.float32).astype(jnp.bfloat16)
    absorbed = jnp.einsum("aub,us->asb", edge, layer, preferred_element_type=jnp.float32).astype(jnp.bfloat16)
    proj3 = projector.reshape(edge.shape[0], layer.shape[0], projector.shape[1])
    moved_proj = lax.all_to_all(proj3, "row", split_axis=1, concat_axis=0, tiled=True)
    moved_edge = lax.all_to_all(absorbed, "row", split_axis=1, concat_axis=0, tiled=True)
    moved_proj = lax.all_gather(moved_proj, "col", axis=2, tiled=True)
    middle = jnp.einsum("asc,asb->scb", moved_proj, moved_edge, preferred_element_type=jnp.float32)
    middle = (middle * moved_edge.shape[0] ** -0.5).astype(jnp.bfloat16)
    regrouped = lax.all_to_all(middle, "row", split_axis=1, concat_axis=0, tiled=True)
    new_edge = jnp.einsum("ts,scb->ctb", layer, regrouped, preferred_element_type=jnp.float32)
    return new_edge.astype(jnp.bfloat16)


def select_columns(vectors, row_count, begin, size):
    new_count = vectors.shape[1]
    per_row = new_count // row_count
    j = lax.broadcasted_iota(jnp.int32, (new_count, row_count * size), 1)
    c = lax.broadcasted_iota(jnp.int32, (new_count, row_count * size), 0)
    chosen = (c == (j // size) * per_row + begin + j % size).astype(jnp.bfloat16)
    return jnp.dot(vectors, chosen, preferred_element_type=jnp.float32).astype(jnp.bfloat16)


def lined(row_count, half_system, vectors, edge, ket, bra):
    lines = row_count // 2
    row, col = lax.axis_index("row"), lax.axis_index("col")
    z, y = row // 2, row % 2
    ring = [(r, (r + 2) % row_count) for r in range(row_count)]
    pair = [(r, r ^ 1) for r in range(row_count)]

    def move(value, links, axis="row"):
        return lax.ppermute(value, axis, links)

    def exchange(value):
        return lax.all_to_all(value, "row", split_axis=0, concat_axis=0, tiled=True)

    depth = vectors.shape[0]

    def dots(at, jobs, part=None, last=None):
        return block_dots(half_system, table, at, depth, jobs, part, last)

    per_row = vectors.shape[1] // row_count
    size = per_row // 2
    own_a, own_b = [select_columns(vectors, row_count, i * size, size) for i in range(2)]
    layer = jnp.dot(ket, bra.T, preferred_element_type=jnp.float32).astype(jnp.bfloat16)
    absorbed = jnp.einsum("aub,us->sab", edge, layer, preferred_element_type=jnp.float32).astype(jnp.bfloat16)
    moved_edge = exchange(absorbed)
    left_count = edge.shape[0] // 2
    scale = (edge.shape[0] * row_count) ** -0.5
    blocks = [2 * ((z - k) % lines) + side for k in range(lines) for side in (y, 1 - y)]
    table = lax.optimization_barrier(jnp.stack([col, 1 - col] + blocks).astype(jnp.int32))
    same, cross = [BLOCKS + 2 * k for k in range(lines)], [BLOCKS + 2 * k + 1 for k in range(lines)]

    def around(own):
        along = [own]
        for _ in range(1, lines):
            along.append(move(along[-1], ring))
        return along

    def project(total, block, name):
        jobs = [(total, [block])]
        last = held(half_system, table, cross[3], depth, 4 if name == "a" else 8)
        (sent,) = dots([cross[3]], jobs, SENT, last)
        partner = move(sent, SWAP, "col")
        (kept,) = dots([cross[3]], jobs, KEPT, last)
        projector = (kept + partner).astype(jnp.bfloat16).reshape(left_count, -1, kept.shape[1])
        moved = exchange(projector.transpose(1, 0, 2))
        other = move(moved, SWAP, "col")
        middle = middle_of(table, row_count, moved, other, moved_edge, scale)
        regrouped = exchange(middle)
        new_edge = jnp.einsum("ts,scb->ctb", layer, regrouped, preferred_element_type=jnp.float32)
        return new_edge.astype(jnp.bfloat16)

    za = around(own_a)
    ya = [move(block, pair) for block in za]
    y0b = move(own_b, pair)
    zb = around(own_b)
    yb = [y0b] + [move(zb[k], pair) for k in range(1, lines)]
    a, b = dots([same[0]], [(None, [za[0]]), (None, [own_b])])
    a, b = dots([same[1], cross[0]], [(a, [za[1], ya[0]]), (b, [None, y0b])])
    (a,) = dots([same[2], cross[1]], [(a, [za[2], ya[1]])])
    (a,) = dots([same[3], cross[2]], [(a, [za[3], ya[2]])])
    first = project(a, ya[3], "a")
    (b,) = dots([same[1], same[2], cross[1]], [(b, [zb[1], zb[2], yb[1]])])
    (b,) = dots([same[3], cross[2]], [(b, [zb[3], yb[2]])])
    second = project(b, yb[3], "b")
    out = jnp.zeros((2 * size, *first.shape[1:]), first.dtype)
    out = lax.optimization_barrier(lax.dynamic_update_slice(out, first, (0, 0, 0)))
    return lax.dynamic_update_slice(out, second, (size, 0, 0))


def solution(mesh):
    row_count = mesh.shape["row"]
    placed = (
        P(("cell", "row"), "col"),
        P(("cell", "col", "row"), None),
        P(("cell", "row"), None, "col"),
        P("cell", None),
        P("cell", None),
    )

    line_form = row_count == 8

    def per_device(half_system, vectors, edge, ket, bra):
        if not line_form:
            return plain(half_system, vectors, edge, ket, bra)
        return lined(row_count, half_system, vectors, edge, ket, bra)

    return jax.shard_map(
        per_device,
        mesh=mesh,
        in_specs=placed,
        out_specs=P(("cell", "row"), None, "col"),
        check_vma=False,
    )
```
